8 devices in a mesh: rep: 2 (over y, z), dp: 4 (over x, core).
Axes of the slice: x: 2, y: 2, z: 1, core: 2. Of those that a mesh axis runs over, the one named last changes fastest.
Arguments:
- x: bfloat16 [8, 2048, 1280], P(('rep', 'dp')), parts along dimension 0
- dy: bfloat16 [8, 2048, 1280], P(('rep', 'dp')), parts along dimension 0
- wq: bfloat16 [2, 1280, 1280], P(None, 'dp')
- wk: bfloat16 [2, 1280, 256], P(None, 'dp')
- wv: bfloat16 [2, 1280, 256], P(None, 'dp')
- wo: bfloat16 [2, 1280, 1280], P(None, 'dp')
- w_gate: bfloat16 [2, 1280, 3456], P(None, 'dp')
- w_up: bfloat16 [2, 1280, 3456], P(None, 'dp')
- w_down: bfloat16 [2, 3456, 1280], P(None, 'dp')
- m_wq: float32 [2, 1280, 1280], P(None, 'dp')
- m_wk: float32 [2, 1280, 256], P(None, 'dp')
- m_wv: float32 [2, 1280, 256], P(None, 'dp')
- m_wo: float32 [2, 1280, 1280], P(None, 'dp')
- m_w_gate: float32 [2, 1280, 3456], P(None, 'dp')
- m_w_up: float32 [2, 1280, 3456], P(None, 'dp')
- m_w_down: float32 [2, 3456, 1280], P(None, 'dp')
- v_wq: float32 [2, 1280, 1280], P(None, 'dp')
- v_wk: float32 [2, 1280, 256], P(None, 'dp')
- v_wv: float32 [2, 1280, 256], P(None, 'dp')
- v_wo: float32 [2, 1280, 1280], P(None, 'dp')
- v_w_gate: float32 [2, 1280, 3456], P(None, 'dp')
- v_w_up: float32 [2, 1280, 3456], P(None, 'dp')
- v_w_down: float32 [2, 3456, 1280], P(None, 'dp')
Outputs:
- output 1: bfloat16 [4, 1280, 1280], P('rep', 'dp'), parts along dimension 0
- output 2: bfloat16 [4, 1280, 256], P('rep', 'dp'), parts along dimension 0
- output 3: bfloat16 [4, 1280, 256], P('rep', 'dp'), parts along dimension 0
- output 4: bfloat16 [4, 1280, 1280], P('rep', 'dp'), parts along dimension 0
- output 5: bfloat16 [4, 1280, 3456], P('rep', 'dp'), parts along dimension 0
- output 6: bfloat16 [4, 1280, 3456], P('rep', 'dp'), parts along dimension 0
- output 7: bfloat16 [4, 3456, 1280], P('rep', 'dp'), parts along dimension 0
- output 8: float32 [4, 1280, 1280], P('rep', 'dp'), parts along dimension 0
- output 9: float32 [4, 1280, 256], P('rep', 'dp'), parts along dimension 0
- output 10: float32 [4, 1280, 256], P('rep', 'dp'), parts along dimension 0
- output 11: float32 [4, 1280, 1280], P('rep', 'dp'), parts along dimension 0
- output 12: float32 [4, 1280, 3456], P('rep', 'dp'), parts along dimension 0
- output 13: float32 [4, 1280, 3456], P('rep', 'dp'), parts along dimension 0
- output 14: float32 [4, 3456, 1280], P('rep', 'dp'), parts along dimension 0
- output 15: float32 [4, 1280, 1280], P('rep', 'dp'), parts along dimension 0
- output 16: float32 [4, 1280, 256], P('rep', 'dp'), parts along dimension 0
- output 17: float32 [4, 1280, 256], P('rep', 'dp'), parts along dimension 0
- output 18: float32 [4, 1280, 1280], P('rep', 'dp'), parts along dimension 0
- output 19: float32 [4, 1280, 3456], P('rep', 'dp'), parts along dimension 0
- output 20: float32 [4, 1280, 3456], P('rep', 'dp'), parts along dimension 0
- output 21: float32 [4, 3456, 1280], P('rep', 'dp'), parts along dimension 0
There are 2 independent parts. The reference program is written for one: setup_inputs(seed, part) draws one part's arguments, and reference() takes and returns one part's arrays. A program takes and returns all parts, laid end to end along the dimension named above; an argument that names none is the same for every part.
All inputs are finite; a program needn't handle non-finite values.
Results may differ from the reference program's by a relative error of at most 0.0271.
Values are sent between devices in bfloat16 or wider.
A program may use at most 2 GiB of HBM per device.

```python
import jax
import jax.numpy as jnp
from jax import lax

SEQUENCES = 4
TOKENS = 2048
D = 1280
HEADS = 10
KV_HEADS = 2
HEAD = 128
FF = 3456
LAYERS = 2
THETA = 10000
NAMES = ("wq", "wk", "wv", "wo", "w_gate", "w_up", "w_down")
SHAPES = {
    "wq": (LAYERS, D, HEADS * HEAD),
    "wk": (LAYERS, D, KV_HEADS * HEAD),
    "wv": (LAYERS, D, KV_HEADS * HEAD),
    "wo": (LAYERS, HEADS * HEAD, D),
    "w_gate": (LAYERS, D, FF),
    "w_up": (LAYERS, D, FF),
    "w_down": (LAYERS, FF, D),
}


def bump(key, n, height):
    away = (jnp.arange(n, dtype=jnp.int32) - jax.random.randint(key, (), 0, n, jnp.int32)) % n
    return jnp.where(away < n // 8, height, 1.0)


def together(key, own, strength):
    shared = jax.random.normal(key, own.shape[1:], jnp.float32)
    return (own + strength * shared) * lax.rsqrt(1 + strength * strength)


def setup_inputs(seed: int = 0, part: int = 0) -> dict:
    kx, kdy, ka, kb, kz, kf, kh, kl, *keys = jax.random.split(jax.random.key(seed), 8 + 3 * len(NAMES))
    kx, kdy, ka, kb = (jax.random.fold_in(k, part) for k in (kx, kdy, ka, kb))
    kw, km, kv = (keys[i::3] for i in range(3))
    shape = (SEQUENCES, TOKENS, D)
    much_x, much_dy = jax.random.uniform(kz, (2,), jnp.float32, 0.0, 1.0)
    loud = 2.0 ** jax.random.uniform(jax.random.fold_in(kz, 1), (), jnp.float32, -1.0, 2.0)
    layers = 2.0 ** jax.random.uniform(kl, (LAYERS, 1, 1), jnp.float32, -1.0, 1.0)
    times = {"wq": 1.0, "wk": 1.0, "wv": 2.0, "wo": layers, "w_gate": 1.0, "w_up": bump(kh, FF, 4.0), "w_down": layers}
    x = together(ka, jax.random.normal(kx, shape, jnp.float32), much_x) * bump(kf, D, 4.0)
    dy = together(kb, jax.random.normal(kdy, shape, jnp.float32), much_dy)
    drawn = {"x": x.astype(jnp.bfloat16), "dy": (loud * dy * (SEQUENCES * TOKENS) ** -0.5).astype(jnp.bfloat16)}
    for key, name in zip(kw, NAMES, strict=True):
        drawn[name] = (jax.random.normal(key, SHAPES[name], jnp.float32) * SHAPES[name][1] ** -0.5 * times[name]).astype(jnp.bfloat16)
    for key, name in zip(km, NAMES, strict=True):
        drawn[f"m_{name}"] = 0.1 * jax.random.normal(key, SHAPES[name], jnp.float32)
    for key, name in zip(kv, NAMES, strict=True):
        drawn[f"v_{name}"] = loud * loud * jax.random.uniform(key, SHAPES[name], jnp.float32, 0.2, 0.6)
    return drawn


def matmul(a, w):
    return jnp.dot(a, w, preferred_element_type=jnp.float32).astype(jnp.bfloat16)


def normed(h):
    wide = h.astype(jnp.float32)
    scale = lax.rsqrt(jnp.mean(wide**2, -1, keepdims=True) + 1e-6)
    return (wide * scale).astype(jnp.bfloat16)


def turned(t, theta):
    half = t.shape[-1] // 2
    angle = jnp.arange(t.shape[0], dtype=jnp.float32)[:, None] * theta ** (-jnp.arange(half, dtype=jnp.float32) / half)
    cos, sin = jnp.cos(angle)[:, None], jnp.sin(angle)[:, None]
    a, b = t[..., :half].astype(jnp.float32), t[..., half:].astype(jnp.float32)
    return jnp.concatenate([a * cos - b * sin, b * cos + a * sin], -1).astype(jnp.bfloat16)


def seen_by(q, k, v):
    tokens, kv = q.shape[0], k.shape[1]
    q = q.reshape(tokens, kv, -1, q.shape[-1])
    scores = jnp.einsum("tgsd,ugd->gstu", q.astype(jnp.float32), k.astype(jnp.float32)) * q.shape[-1] ** -0.5
    place = jnp.arange(tokens)
    weights = jax.nn.softmax(jnp.where(place[:, None] >= place, scores, -jnp.inf), -1).astype(jnp.bfloat16)
    return jnp.einsum("gstu,ugd->tgsd", weights.astype(jnp.float32), v.astype(jnp.float32)).astype(jnp.bfloat16).reshape(tokens, -1)


def layer(h, w):
    a = normed(h)
    q, k = (turned(matmul(a, w[name]).reshape(h.shape[0], -1, HEAD), THETA) for name in ("wq", "wk"))
    h = h + matmul(seen_by(q, k, matmul(a, w["wv"]).reshape(h.shape[0], -1, HEAD)), w["wo"])
    b = normed(h)
    gate = jnp.dot(b, w["w_gate"], preferred_element_type=jnp.float32)
    up = jnp.dot(b, w["w_up"], preferred_element_type=jnp.float32)
    return h + matmul((jax.nn.silu(gate) * up).astype(jnp.bfloat16), w["w_down"])


def adamw(w, m, v, g):
    m = 0.9 * m + 0.1 * g
    v = 0.95 * v + 0.05 * g * g
    step = m * lax.rsqrt(v + 1e-8) + 0.1 * w
    return (w - 0.02 * step).astype(jnp.bfloat16), m, v


def stack(weights, h):
    return lax.scan(lambda h, w: (layer(h, w), None), h, weights)[0]


def reference(x, dy, wq, wk, wv, wo, w_gate, w_up, w_down, m_wq, m_wk, m_wv, m_wo, m_w_gate, m_w_up, m_w_down, v_wq, v_wk, v_wv, v_wo, v_w_gate, v_w_up, v_w_down):
    weights = dict(zip(NAMES, (wq, wk, wv, wo, w_gate, w_up, w_down), strict=True))

    def take(so_far, sequence):
        h, by_y = sequence
        _, back = jax.vjp(stack, weights, h)
        by_weights, by_h = back(by_y)
        return jax.tree.map(lambda total, term: total + term.astype(jnp.float32), so_far, by_weights), by_h

    none_yet = {name: jnp.zeros(w.shape, jnp.float32) for name, w in weights.items()}
    by_weights, by_x = lax.scan(take, none_yet, (x, dy))
    gradients = [by_weights[name].astype(jnp.bfloat16).astype(jnp.float32) for name in NAMES]
    first = (m_wq, m_wk, m_wv, m_wo, m_w_gate, m_w_up, m_w_down)
    second = (v_wq, v_wk, v_wv, v_wo, v_w_gate, v_w_up, v_w_down)
    new = [adamw(weights[name].astype(jnp.float32), m, v, g) for name, m, v, g in zip(NAMES, first, second, gradients, strict=True)]
    return tuple(one[which] for which in range(3) for one in new)
```

```python
import functools

import jax
import jax.numpy as jnp
from jax import lax
from jax.experimental import pallas as pl
from jax.experimental.pallas import tpu as pltpu
from jax.sharding import PartitionSpec as P

HEAD = 128
THETA = 10000
HEADS, KV = 10, 2
GROUP = HEADS // KV
LOG2E = 1.4426950408889634
NEG = -1e30
HIDDEN = 2 * NEG
VMEM = 60 * 2**20
BF, F32 = jnp.bfloat16, jnp.float32
QW, KW = HEADS * HEAD, KV * HEAD


def _dot(a, b, ca, cb):
    return lax.dot_general(a, b, (((ca,), (cb,)), ((), ())), preferred_element_type=F32)


def _turn(x, cos, sin):
    x = x.astype(F32)
    return x * cos + pltpu.roll(x, HEAD // 2, 1) * sin


def _turn_back(x, cos, sin):
    x = x.astype(F32)
    return x * cos - pltpu.roll(x, HEAD // 2, 1) * sin


def _head(ref, n):
    return ref[:, n * HEAD : (n + 1) * HEAD]


def _gap(bk, cols, bq):
    return lax.rem(lax.broadcasted_iota(jnp.int32, (bk, cols), 1), bq) - lax.broadcasted_iota(jnp.int32, (bk, cols), 0)


def _load_keys(k_ref, ck_ref, sk_ref, k_s):
    for i in range(KV):
        k_s[i] = _turn(_head(k_ref, i), ck_ref[...], sk_ref[...]).astype(BF)


def _load_queries(q_ref, cq_ref, sq_ref, q_s, bq):
    for i in range(KV):
        for n in range(GROUP):
            q_s[i, n * bq : (n + 1) * bq, :] = _turn(_head(q_ref, i * GROUP + n), cq_ref[...], sq_ref[...]).astype(BF)


def _attn_fwd(q_ref, k_ref, v_ref, cq_ref, sq_ref, ck_ref, sk_ref, o_ref, lse_ref, q_s, k_s, v_s, top_s, mix_s, gap_s, *, bq, bk, wide):
    cols, s = GROUP * bq, k_ref.shape[0]
    iq = pl.program_id(0)
    scale = HEAD**-0.5
    e = scale * LOG2E
    pieces = [(i, at) for i in range(KV) for at in range(0, cols, wide)]

    @pl.when(iq == 0)
    def _():
        gap_s[...] = _gap(bk, cols, bq)
        _load_keys(k_ref, ck_ref, sk_ref, k_s)
        for i in range(KV):
            v_s[i, :HEAD, :] = _head(v_ref, i).T
            v_s[i, HEAD:, :] = jnp.ones((8, s), BF)

    _load_queries(q_ref, cq_ref, sq_ref, q_s, bq)
    top_s[...] = jnp.full(top_s.shape, NEG, F32)
    mix_s[...] = jnp.zeros(mix_s.shape, F32)

    def block(j, masked):
        here = pl.ds(pl.multiple_of(j * bk, bk), bk)
        scores = [_dot(k_s[i, here, :], q_s[i, at : at + wide, :], 1, 1) for i, at in pieces]
        if masked:
            ok = gap_s[...] >= j * bk - iq * bq
        weights, keeps = [], []
        for (i, at), x in zip(pieces, scores):
            if masked:
                x = jnp.where(ok[:, at : at + wide], x, HIDDEN)
            old = top_s[i : i + 1, at : at + wide]
            top = jnp.maximum(old, x.max(axis=0, keepdims=True))
            top_s[i : i + 1, at : at + wide] = top
            weights.append(jnp.exp2((x - top) * e).astype(BF))
            keeps.append(jnp.exp2((old - top) * e))
        for (i, at), p, keep in zip(pieces, weights, keeps):
            mix_s[i, :, at : at + wide] = mix_s[i, :, at : at + wide] * keep + _dot(v_s[i, :, here], p, 1, 0)

    whole, last = lax.div(iq * bq, bk), lax.div(iq * bq + bq + bk - 1, bk)
    lax.fori_loop(0, whole, lambda j, _: block(j, False), None)
    lax.fori_loop(whole, last, lambda j, _: block(j, True), None)

    for i in range(KV):
        top, total = top_s[i : i + 1, :], mix_s[i, HEAD : HEAD + 1, :]
        out = (mix_s[i, :HEAD, :] * (1 / total)).T.astype(BF)
        lse = top * scale + jnp.log(total)
        for n in range(GROUP):
            at = i * GROUP + n
            o_ref[:, at * HEAD : (at + 1) * HEAD] = out[n * bq : (n + 1) * bq, :]
            lse_ref[at : at + 1, :] = lse[:, n * bq : (n + 1) * bq]


def _attn_bwd(q_ref, k_ref, v_ref, o_ref, do_ref, lse_ref, cq_ref, sq_ref, ck_ref, sk_ref, d_ref, q_s, do_s, k_s, kt_s, dq_s, dk_s, dv_s, gap_s,
              *, bq, bk, wide):
    cols = GROUP * bq
    iq = pl.program_id(0)
    scale = HEAD**-0.5
    e = scale * LOG2E
    pieces = [(i, at) for i in range(KV) for at in range(0, cols, wide)]

    @pl.when(iq == 0)
    def _():
        gap_s[...] = _gap(bk, cols, bq)
        dk_s[...] = jnp.zeros_like(dk_s)
        dv_s[...] = jnp.zeros_like(dv_s)
        _load_keys(k_ref, ck_ref, sk_ref, k_s)
        for i in range(KV):
            kt_s[i] = k_s[i].T

    _load_queries(q_ref, cq_ref, sq_ref, q_s, bq)
    dq_s[...] = jnp.zeros_like(dq_s)
    lses, deltas = [], []
    for i in range(KV):
        row, delta = [], []
        for n in range(GROUP):
            at = i * GROUP + n
            do = _head(do_ref, at)
            do_s[i, n * bq : (n + 1) * bq, :] = do
            row.append(lse_ref[at : at + 1, :] * LOG2E)
            delta.append((do.astype(F32) * _head(o_ref, at).astype(F32)).T.sum(axis=0, keepdims=True))
        lses.append(jnp.concatenate(row, axis=1))
        deltas.append(jnp.concatenate(delta, axis=1))

    def block(j, masked):
        here = pl.ds(pl.multiple_of(j * bk, bk), bk)
        qs = [q_s[i, at : at + wide, :] for i, at in pieces]
        dos = [do_s[i, at : at + wide, :] for i, at in pieces]
        scores = [_dot(k_s[i, here, :], x, 1, 1) for (i, _), x in zip(pieces, qs)]
        dps = [_dot(v_ref[here, i * HEAD : (i + 1) * HEAD], x, 1, 1) for (i, _), x in zip(pieces, dos)]
        if masked:
            ok = gap_s[...] >= j * bk - iq * bq
        for n, (i, at) in enumerate(pieces):
            p = jnp.exp2(scores[n] * e - lses[i][:, at : at + wide])
            if masked:
                p = jnp.where(ok[:, at : at + wide], p, 0.0)
            ds = (p * (dps[n] - deltas[i][:, at : at + wide])).astype(BF)
            dv_s[i, here, :] += _dot(p.astype(BF), dos[n], 1, 0)
            dk_s[i, here, :] += _dot(ds, qs[n], 1, 0)
            dq_s[i, :, at : at + wide] += _dot(kt_s[i, :, here], ds, 1, 0)

    whole, last = lax.div(iq * bq, bk), lax.div(iq * bq + bq + bk - 1, bk)
    lax.fori_loop(0, whole, lambda j, _: block(j, False), None)
    lax.fori_loop(whole, last, lambda j, _: block(j, True), None)
    rows = pl.ds(pl.multiple_of(iq * bq, bq), bq)
    for i in range(KV):
        dq = (dq_s[i] * scale).T.astype(BF)
        for n in range(GROUP):
            at = i * GROUP + n
            d_ref[rows, at * HEAD : (at + 1) * HEAD] = _turn_back(dq[n * bq : (n + 1) * bq, :], cq_ref[...], sq_ref[...]).astype(BF)

    @pl.when(iq == pl.num_programs(0) - 1)
    def _():
        for i in range(KV):
            dk = (dk_s[i] * scale).astype(BF)
            d_ref[:, QW + i * HEAD : QW + (i + 1) * HEAD] = _turn_back(dk, ck_ref[...], sk_ref[...]).astype(BF)
            d_ref[:, QW + KW + i * HEAD : QW + KW + (i + 1) * HEAD] = dv_s[i].astype(BF)


def _attn_specs(s, bq):
    q = pl.BlockSpec((bq, QW), lambda i: (i, 0))
    k = pl.BlockSpec((s, KW), lambda i: (0, QW // KW))
    v = pl.BlockSpec((s, KW), lambda i: (0, QW // KW + 1))
    part = pl.BlockSpec((bq, HEAD), lambda i: (i, 0))
    whole = pl.BlockSpec((s, HEAD), lambda i: (0, 0))
    stat = pl.BlockSpec((HEADS, bq), lambda i: (0, i))
    return q, k, v, part, whole, stat


def attend(qkv, cos, sin, bq=512, bk=512, wide=512):
    s = qkv.shape[0]
    q, k, v, part, whole, stat = _attn_specs(s, bq)
    cols = GROUP * bq
    return pl.pallas_call(
        functools.partial(_attn_fwd, bq=bq, bk=bk, wide=wide),
        grid=(s // bq,),
        in_specs=[q, k, v, part, part, whole, whole],
        out_specs=[q, stat],
        out_shape=[jax.ShapeDtypeStruct((s, QW), BF), jax.ShapeDtypeStruct((HEADS, s), F32)],
        scratch_shapes=[pltpu.VMEM((KV, cols, HEAD), BF), pltpu.VMEM((KV, s, HEAD), BF), pltpu.VMEM((KV, HEAD + 8, s), BF),
                        pltpu.VMEM((KV, cols), F32), pltpu.VMEM((KV, HEAD + 8, cols), F32), pltpu.VMEM((bk, cols), jnp.int32)],
        compiler_params=pltpu.CompilerParams(dimension_semantics=("arbitrary",), vmem_limit_bytes=VMEM),
        cost_estimate=pl.CostEstimate(flops=40 * 10**9, transcendentals=HEADS * s * s, bytes_accessed=8 * s * QW),
        name="attend",
    )(qkv, qkv, qkv, cos, sin, cos, sin)


def attend_bwd(qkv, o, do, lse, cos, sin, bq=256, bk=256, wide=256):
    s = qkv.shape[0]
    q, k, v, part, whole, stat = _attn_specs(s, bq)
    cols = GROUP * bq
    return pl.pallas_call(
        functools.partial(_attn_bwd, bq=bq, bk=bk, wide=wide),
        grid=(s // bq,),
        in_specs=[q, k, v, q, q, stat, part, part, whole, whole],
        out_specs=pl.BlockSpec((s, QW + 2 * KW), lambda i: (0, 0)),
        out_shape=jax.ShapeDtypeStruct((s, QW + 2 * KW), BF),
        scratch_shapes=[pltpu.VMEM((KV, cols, HEAD), BF), pltpu.VMEM((KV, cols, HEAD), BF), pltpu.VMEM((KV, s, HEAD), BF),
                        pltpu.VMEM((KV, HEAD, s), BF), pltpu.VMEM((KV, HEAD, cols), F32), pltpu.VMEM((KV, s, HEAD), F32),
                        pltpu.VMEM((KV, s, HEAD), F32), pltpu.VMEM((bk, cols), jnp.int32)],
        compiler_params=pltpu.CompilerParams(dimension_semantics=("arbitrary",), vmem_limit_bytes=VMEM),
        cost_estimate=pl.CostEstimate(flops=80 * 10**9, transcendentals=HEADS * s * s, bytes_accessed=16 * s * QW),
        name="attend_bwd",
    )(qkv, qkv, qkv, o, do, lse, cos, sin, cos, sin)


def _adam(count, *refs):
    ws, ms, vs, gs = (refs[i * count : (i + 1) * count] for i in range(4))
    outs = refs[-3 * count :]
    for i in range(count):
        g = gs[i][...].astype(F32)
        w = ws[i][0].astype(F32)
        m = 0.9 * ms[i][0] + 0.1 * g
        v = 0.95 * vs[i][0] + 0.05 * g * g
        outs[i][0] = (w - 0.02 * (m * lax.rsqrt(v + 1e-8) + 0.1 * w)).astype(BF)
        outs[count + i][0] = m
        outs[2 * count + i][0] = v


def adam(number, ws, ms, vs, g, made, steps):
    count, rows = len(ws), g.shape[0]
    br = rows // steps
    layer = [pl.BlockSpec((1, br, w.shape[2]), lambda i: (number, i, 0)) for w in ws]
    at, gspecs = 0, []
    for w in ws:
        n = w.shape[2]
        gspecs.append(pl.BlockSpec((br, n), functools.partial(lambda i, c: (i, c), c=at // n)))
        at += n
    made = () if made is None else made
    elements = rows * at
    return pl.pallas_call(
        functools.partial(_adam, count),
        grid=(steps,),
        in_specs=layer * 3 + gspecs + [pl.BlockSpec(memory_space=pl.ANY)] * len(made),
        out_specs=layer * 3,
        out_shape=[jax.ShapeDtypeStruct(w.shape, t) for t in (BF, F32, F32) for w in ws],
        input_output_aliases={4 * count + i: i for i in range(len(made))},
        compiler_params=pltpu.CompilerParams(dimension_semantics=("arbitrary",), vmem_limit_bytes=40 * 2**20),
        cost_estimate=pl.CostEstimate(flops=2000 * elements, transcendentals=elements, bytes_accessed=22 * elements),
        name="adam",
    )(*ws, *ms, *vs, *([g] * count), *made)


def matmul(a, w):
    return jnp.dot(a, w, preferred_element_type=F32).astype(BF)


def normed(h):
    wide = h.astype(F32)
    scale = lax.rsqrt(jnp.mean(wide**2, -1, keepdims=True) + 1e-6)
    return (wide * scale).astype(BF), scale


def by_norm(h, scale, d):
    wide, d = h.astype(F32), d.astype(F32)
    return (scale * d - wide * (scale**3 * jnp.mean(wide * d, -1, keepdims=True))).astype(BF)


def order(*arrays):
    return lax.optimization_barrier(arrays)


def solution(mesh):
    def whole(shard):
        half = shard.shape[0] // 2
        mine = lax.dynamic_slice_in_dim(shard, lax.axis_index("rep") * half, half, 0)
        return lax.all_gather(mine, ("dp", "rep"), axis=0, tiled=True)

    def summed(g):
        return lax.psum_scatter(g, "dp", scatter_dimension=0, tiled=True)

    def step(x, dy, *arrays):
        w, m, v = (arrays[i : i + 7] for i in (0, 7, 14))
        layers = w[0].shape[0]
        tokens = x.shape[1]
        half = HEAD // 2
        angle = jnp.arange(tokens, dtype=F32)[:, None] * THETA ** (-jnp.arange(half, dtype=F32) / half)
        cos, sin = jnp.cos(angle), jnp.sin(angle)
        cos, sin = jnp.concatenate([cos, cos], 1), jnp.concatenate([-sin, sin], 1)

        full = []
        for n in range(layers):
            qkv = jnp.concatenate([w[0][n], w[1][n], w[2][n]], axis=1)
            full.append([whole(s) for s in (qkv, w[3][n], w[4][n], w[5][n], w[6][n])])

        h, kept = x[0], []
        for n in range(layers):
            wqkv, wo, wg, wu, wd = full[n]
            a, sa = normed(h)
            qkv = matmul(a, wqkv)
            o, lse = attend(qkv, cos, sin)
            h1 = h + matmul(o, wo)
            b, sb = normed(h1)
            gate = jnp.dot(b, wg, preferred_element_type=F32)
            up = jnp.dot(b, wu, preferred_element_type=F32)
            act = (jax.nn.silu(gate) * up).astype(BF)
            kept.append((h, a, sa, qkv, o, lse, h1, b, sb, gate, up, act))
            if n < layers - 1:
                h = h1 + matmul(act, wd)

        d = dy[0]
        made = [None] * 5
        groups = [(0, 1, 2), (3,), (4,), (5,), (6,)]

        def take(n, k, g):
            made[k] = adam(n, *[[t[i] for i in groups[k]] for t in (w, m, v)], g, made[k], 5 if k < 4 else 9)

        for n in reversed(range(layers)):
            wqkv, wo, wg, wu, wd = full[n]
            h, a, sa, qkv, o, lse, h1, b, sb, gate, up, act = kept[n]
            gwd, d, act = order(_dot(act, d, 0, 0).astype(BF), d, act)
            gwd = summed(gwd)
            dact = _dot(d, wd, 1, 1).astype(BF).astype(F32)
            sig = jax.nn.sigmoid(gate)
            dup = (dact * (gate * sig)).astype(BF)
            dgate = (dact * up * (sig * (1 + gate * (1 - sig)))).astype(BF)
            dgate, dup = order(dgate, dup)
            gwg, dgate, dup = order(_dot(b, dgate, 0, 0).astype(BF), dgate, dup)
            gwg = summed(gwg)
            gwu, dgate, dup = order(_dot(b, dup, 0, 0).astype(BF), dgate, dup)
            gwu = summed(gwu)
            db = _dot(dgate, wg, 1, 1) + _dot(dup, wu, 1, 1)
            d1 = d + by_norm(h1, sb, db)
            gwo, d1 = order(_dot(o, d1, 0, 0).astype(BF), d1)
            gwo = summed(gwo)
            do = _dot(d1, wo, 1, 1).astype(BF)
            dqkv = attend_bwd(qkv, o, do, lse, cos, sin)
            gq, dqkv = order(_dot(a, dqkv, 0, 0).astype(BF), dqkv)
            gq = summed(gq)
            if n > 0:
                da = _dot(dqkv, wqkv, 1, 1)
                d = d1 + by_norm(h, sa, da)
            for k, g in ((4, gwd), (2, gwg), (3, gwu), (1, gwo), (0, gq)):
                take(n, k, g)
        flat = {i: [made[k][t * len(groups[k]) + j] for t in range(3)] for k in range(5) for j, i in enumerate(groups[k])}
        return tuple(flat[i][t] for t in range(3) for i in range(7))

    states, cut = P(("rep", "dp"), None, None), P(None, "dp", None)
    return jax.shard_map(
        step,
        mesh=mesh,
        in_specs=(states, states) + (cut,) * 21,
        out_specs=(P("rep", "dp", None),) * 21,
        check_vma=False,
    )
```

```python
import functools

import jax
import jax.numpy as jnp
from jax import lax
from jax.experimental import pallas as pl
from jax.experimental.pallas import tpu as pltpu
from jax.sharding import PartitionSpec as P

HEAD = 128
THETA = 10000
HEADS, KV = 10, 2
GROUP = HEADS // KV
LOG2E = 1.4426950408889634
NEG = -1e30
HIDDEN = 2 * NEG
VMEM = 60 * 2**20
BF, F32 = jnp.bfloat16, jnp.float32
QW, KW = HEADS * HEAD, KV * HEAD


def _dot(a, b, ca, cb):
    return lax.dot_general(a, b, (((ca,), (cb,)), ((), ())), preferred_element_type=F32)


def _turn(x, cos, sin):
    x = x.astype(F32)
    return x * cos + pltpu.roll(x, HEAD // 2, 1) * sin


def _turn_back(x, cos, sin):
    x = x.astype(F32)
    return x * cos - pltpu.roll(x, HEAD // 2, 1) * sin


def _head(ref, n):
    return ref[:, n * HEAD : (n + 1) * HEAD]


def _gap(bk, cols, bq):
    return lax.rem(lax.broadcasted_iota(jnp.int32, (bk, cols), 1), bq) - lax.broadcasted_iota(jnp.int32, (bk, cols), 0)


def _load_keys(k_ref, ck_ref, sk_ref, k_s):
    for i in range(KV):
        k_s[i] = _turn(_head(k_ref, i), ck_ref[...], sk_ref[...]).astype(BF)


def _load_queries(q_ref, cq_ref, sq_ref, q_s, bq):
    for i in range(KV):
        for n in range(GROUP):
            q_s[i, n * bq : (n + 1) * bq, :] = _turn(_head(q_ref, i * GROUP + n), cq_ref[...], sq_ref[...]).astype(BF)


def _attn_fwd(q_ref, k_ref, v_ref, cq_ref, sq_ref, ck_ref, sk_ref, o_ref, lse_ref, q_s, k_s, v_s, top_s, mix_s, gap_s, *, bq, bk, wide):
    cols, s = GROUP * bq, k_ref.shape[0]
    iq = pl.program_id(0)
    scale = HEAD**-0.5
    e = scale * LOG2E
    pieces = [(i, at) for i in range(KV) for at in range(0, cols, wide)]

    @pl.when(iq == 0)
    def _():
        gap_s[...] = _gap(bk, cols, bq)
        _load_keys(k_ref, ck_ref, sk_ref, k_s)
        for i in range(KV):
            v_s[i, :HEAD, :] = _head(v_ref, i).T
            v_s[i, HEAD:, :] = jnp.ones((8, s), BF)

    _load_queries(q_ref, cq_ref, sq_ref, q_s, bq)
    top_s[...] = jnp.full(top_s.shape, NEG, F32)
    mix_s[...] = jnp.zeros(mix_s.shape, F32)

    def block(j, masked):
        here = pl.ds(pl.multiple_of(j * bk, bk), bk)
        scores = [_dot(k_s[i, here, :], q_s[i, at : at + wide, :], 1, 1) for i, at in pieces]
        if masked:
            ok = gap_s[...] >= j * bk - iq * bq
        weights, keeps = [], []
        for (i, at), x in zip(pieces, scores):
            if masked:
                x = jnp.where(ok[:, at : at + wide], x, HIDDEN)
            old = top_s[i : i + 1, at : at + wide]
            top = jnp.maximum(old, x.max(axis=0, keepdims=True))
            top_s[i : i + 1, at : at + wide] = top
            weights.append(jnp.exp2((x - top) * e).astype(BF))
            keeps.append(jnp.exp2((old - top) * e))
        for (i, at), p, keep in zip(pieces, weights, keeps):
            mix_s[i, :, at : at + wide] = mix_s[i, :, at : at + wide] * keep + _dot(v_s[i, :, here], p, 1, 0)

    whole, last = lax.div(iq * bq, bk), lax.div(iq * bq + bq + bk - 1, bk)
    lax.fori_loop(0, whole, lambda j, _: block(j, False), None)
    lax.fori_loop(whole, last, lambda j, _: block(j, True), None)

    for i in range(KV):
        top, total = top_s[i : i + 1, :], mix_s[i, HEAD : HEAD + 1, :]
        out = (mix_s[i, :HEAD, :] * (1 / total)).T.astype(BF)
        lse = top * scale + jnp.log(total)
        for n in range(GROUP):
            at = i * GROUP + n
            o_ref[:, at * HEAD : (at + 1) * HEAD] = out[n * bq : (n + 1) * bq, :]
            lse_ref[at : at + 1, :] = lse[:, n * bq : (n + 1) * bq]


def _attn_bwd(q_ref, k_ref, v_ref, o_ref, do_ref, lse_ref, cq_ref, sq_ref, ck_ref, sk_ref, d_ref, q_s, do_s, k_s, kt_s, dq_s, dk_s, dv_s, gap_s,
              *, bq, bk, wide):
    cols = GROUP * bq
    iq = pl.program_id(0)
    scale = HEAD**-0.5
    e = scale * LOG2E
    pieces = [(i, at) for i in range(KV) for at in range(0, cols, wide)]

    @pl.when(iq == 0)
    def _():
        gap_s[...] = _gap(bk, cols, bq)
        dk_s[...] = jnp.zeros_like(dk_s)
        dv_s[...] = jnp.zeros_like(dv_s)
        _load_keys(k_ref, ck_ref, sk_ref, k_s)
        for i in range(KV):
            kt_s[i] = k_s[i].T

    _load_queries(q_ref, cq_ref, sq_ref, q_s, bq)
    dq_s[...] = jnp.zeros_like(dq_s)
    lses, deltas = [], []
    for i in range(KV):
        row, delta = [], []
        for n in range(GROUP):
            at = i * GROUP + n
            do = _head(do_ref, at)
            do_s[i, n * bq : (n + 1) * bq, :] = do
            row.append(lse_ref[at : at + 1, :] * LOG2E)
            delta.append((do.astype(F32) * _head(o_ref, at).astype(F32)).T.sum(axis=0, keepdims=True))
        lses.append(jnp.concatenate(row, axis=1))
        deltas.append(jnp.concatenate(delta, axis=1))

    def block(j, masked):
        here = pl.ds(pl.multiple_of(j * bk, bk), bk)
        qs = [q_s[i, at : at + wide, :] for i, at in pieces]
        dos = [do_s[i, at : at + wide, :] for i, at in pieces]
        scores = [_dot(k_s[i, here, :], x, 1, 1) for (i, _), x in zip(pieces, qs)]
        dps = [_dot(v_ref[here, i * HEAD : (i + 1) * HEAD], x, 1, 1) for (i, _), x in zip(pieces, dos)]
        if masked:
            ok = gap_s[...] >= j * bk - iq * bq
        for n, (i, at) in enumerate(pieces):
            p = jnp.exp2(scores[n] * e - lses[i][:, at : at + wide])
            if masked:
                p = jnp.where(ok[:, at : at + wide], p, 0.0)
            ds = (p * (dps[n] - deltas[i][:, at : at + wide])).astype(BF)
            dv_s[i, here, :] += _dot(p.astype(BF), dos[n], 1, 0)
            dk_s[i, here, :] += _dot(ds, qs[n], 1, 0)
            dq_s[i, :, at : at + wide] += _dot(kt_s[i, :, here], ds, 1, 0)

    whole, last = lax.div(iq * bq, bk), lax.div(iq * bq + bq + bk - 1, bk)
    lax.fori_loop(0, whole, lambda j, _: block(j, False), None)
    lax.fori_loop(whole, last, lambda j, _: block(j, True), None)
    rows = pl.ds(pl.multiple_of(iq * bq, bq), bq)
    for i in range(KV):
        dq = (dq_s[i] * scale).T.astype(BF)
        for n in range(GROUP):
            at = i * GROUP + n
            d_ref[rows, at * HEAD : (at + 1) * HEAD] = _turn_back(dq[n * bq : (n + 1) * bq, :], cq_ref[...], sq_ref[...]).astype(BF)

    @pl.when(iq == pl.num_programs(0) - 1)
    def _():
        for i in range(KV):
            dk = (dk_s[i] * scale).astype(BF)
            d_ref[:, QW + i * HEAD : QW + (i + 1) * HEAD] = _turn_back(dk, ck_ref[...], sk_ref[...]).astype(BF)
            d_ref[:, QW + KW + i * HEAD : QW + KW + (i + 1) * HEAD] = dv_s[i].astype(BF)


def _attn_specs(s, bq):
    q = pl.BlockSpec((bq, QW), lambda i: (i, 0))
    k = pl.BlockSpec((s, KW), lambda i: (0, QW // KW))
    v = pl.BlockSpec((s, KW), lambda i: (0, QW // KW + 1))
    part = pl.BlockSpec((bq, HEAD), lambda i: (i, 0))
    whole = pl.BlockSpec((s, HEAD), lambda i: (0, 0))
    stat = pl.BlockSpec((HEADS, bq), lambda i: (0, i))
    return q, k, v, part, whole, stat


def attend(qkv, cos, sin, bq=512, bk=512, wide=512):
    s = qkv.shape[0]
    q, k, v, part, whole, stat = _attn_specs(s, bq)
    cols = GROUP * bq
    return pl.pallas_call(
        functools.partial(_attn_fwd, bq=bq, bk=bk, wide=wide),
        grid=(s // bq,),
        in_specs=[q, k, v, part, part, whole, whole],
        out_specs=[q, stat],
        out_shape=[jax.ShapeDtypeStruct((s, QW), BF), jax.ShapeDtypeStruct((HEADS, s), F32)],
        scratch_shapes=[pltpu.VMEM((KV, cols, HEAD), BF), pltpu.VMEM((KV, s, HEAD), BF), pltpu.VMEM((KV, HEAD + 8, s), BF),
                        pltpu.VMEM((KV, cols), F32), pltpu.VMEM((KV, HEAD + 8, cols), F32), pltpu.VMEM((bk, cols), jnp.int32)],
        compiler_params=pltpu.CompilerParams(dimension_semantics=("arbitrary",), vmem_limit_bytes=VMEM),
        cost_estimate=pl.CostEstimate(flops=40 * 10**9, transcendentals=HEADS * s * s, bytes_accessed=8 * s * QW),
        name="attend",
    )(qkv, qkv, qkv, cos, sin, cos, sin)


def attend_bwd(qkv, o, do, lse, cos, sin, bq=256, bk=256, wide=256):
    s = qkv.shape[0]
    q, k, v, part, whole, stat = _attn_specs(s, bq)
    cols = GROUP * bq
    return pl.pallas_call(
        functools.partial(_attn_bwd, bq=bq, bk=bk, wide=wide),
        grid=(s // bq,),
        in_specs=[q, k, v, q, q, stat, part, part, whole, whole],
        out_specs=pl.BlockSpec((s, QW + 2 * KW), lambda i: (0, 0)),
        out_shape=jax.ShapeDtypeStruct((s, QW + 2 * KW), BF),
        scratch_shapes=[pltpu.VMEM((KV, cols, HEAD), BF), pltpu.VMEM((KV, cols, HEAD), BF), pltpu.VMEM((KV, s, HEAD), BF),
                        pltpu.VMEM((KV, HEAD, s), BF), pltpu.VMEM((KV, HEAD, cols), F32), pltpu.VMEM((KV, s, HEAD), F32),
                        pltpu.VMEM((KV, s, HEAD), F32), pltpu.VMEM((bk, cols), jnp.int32)],
        compiler_params=pltpu.CompilerParams(dimension_semantics=("arbitrary",), vmem_limit_bytes=VMEM),
        cost_estimate=pl.CostEstimate(flops=80 * 10**9, transcendentals=HEADS * s * s, bytes_accessed=16 * s * QW),
        name="attend_bwd",
    )(qkv, qkv, qkv, o, do, lse, cos, sin, cos, sin)


def _adam(count, *refs):
    ws, ms, vs, gs = (refs[i * count : (i + 1) * count] for i in range(4))
    outs = refs[-3 * count :]
    for i in range(count):
        g = gs[i][...].astype(F32)
        w = ws[i][0].astype(F32)
        m = 0.9 * ms[i][0] + 0.1 * g
        v = 0.95 * vs[i][0] + 0.05 * g * g
        outs[i][0] = (w - 0.02 * (m * lax.rsqrt(v + 1e-8) + 0.1 * w)).astype(BF)
        outs[count + i][0] = m
        outs[2 * count + i][0] = v


def adam(number, ws, ms, vs, g, made, steps):
    count, rows = len(ws), g.shape[0]
    br = rows // steps
    layer = [pl.BlockSpec((1, br, w.shape[2]), lambda i: (number, i, 0)) for w in ws]
    at, gspecs = 0, []
    for w in ws:
        n = w.shape[2]
        gspecs.append(pl.BlockSpec((br, n), functools.partial(lambda i, c: (i, c), c=at // n)))
        at += n
    made = () if made is None else made
    elements = rows * at
    return pl.pallas_call(
        functools.partial(_adam, count),
        grid=(steps,),
        in_specs=layer * 3 + gspecs + [pl.BlockSpec(memory_space=pl.ANY)] * len(made),
        out_specs=layer * 3,
        out_shape=[jax.ShapeDtypeStruct(w.shape, t) for t in (BF, F32, F32) for w in ws],
        input_output_aliases={4 * count + i: i for i in range(len(made))},
        compiler_params=pltpu.CompilerParams(dimension_semantics=("arbitrary",), vmem_limit_bytes=40 * 2**20),
        cost_estimate=pl.CostEstimate(flops=2000 * elements, transcendentals=elements, bytes_accessed=22 * elements),
        name="adam",
    )(*ws, *ms, *vs, *([g] * count), *made)


def matmul(a, w):
    return jnp.dot(a, w, preferred_element_type=F32).astype(BF)


def normed(h):
    wide = h.astype(F32)
    scale = lax.rsqrt(jnp.mean(wide**2, -1, keepdims=True) + 1e-6)
    return (wide * scale).astype(BF), scale


def by_norm(h, scale, d):
    wide, d = h.astype(F32), d.astype(F32)
    return (scale * d - wide * (scale**3 * jnp.mean(wide * d, -1, keepdims=True))).astype(BF)


def order(*arrays):
    return lax.optimization_barrier(arrays)


def solution(mesh):
    def whole(shard):
        half = shard.shape[0] // 2
        mine = lax.dynamic_slice_in_dim(shard, lax.axis_index("rep") * half, half, 0)
        return lax.all_gather(mine, ("dp", "rep"), axis=0, tiled=True)

    def summed(g):
        return lax.psum_scatter(g, "dp", scatter_dimension=0, tiled=True)

    def step(x, dy, *arrays):
        w, m, v = (arrays[i : i + 7] for i in (0, 7, 14))
        layers = w[0].shape[0]
        tokens = x.shape[1]
        half = HEAD // 2
        angle = jnp.arange(tokens, dtype=F32)[:, None] * THETA ** (-jnp.arange(half, dtype=F32) / half)
        cos, sin = jnp.cos(angle), jnp.sin(angle)
        cos, sin = jnp.concatenate([cos, cos], 1), jnp.concatenate([-sin, sin], 1)

        full = []
        for n in range(layers):
            qkv = jnp.concatenate([w[0][n], w[1][n], w[2][n]], axis=1)
            full.append([whole(s) for s in (qkv, w[3][n], w[4][n], w[5][n], w[6][n])])

        h, kept = x[0], []
        for n in range(layers):
            wqkv, wo, wg, wu, wd = full[n]
            a, sa = normed(h)
            qkv = matmul(a, wqkv)
            o, lse = attend(qkv, cos, sin)
            h1 = h + matmul(o, wo)
            b, sb = normed(h1)
            gate = jnp.dot(b, wg, preferred_element_type=F32)
            up = jnp.dot(b, wu, preferred_element_type=F32)
            act = (jax.nn.silu(gate) * up).astype(BF)
            kept.append((h, a, sa, qkv, o, lse, h1, b, sb, gate, up, act))
            if n < layers - 1:
                h = h1 + matmul(act, wd)

        d = dy[0]
        made = [None] * 5
        groups = [(0, 1, 2), (3,), (4,), (5,), (6,)]

        def take(n, k, g):
            made[k] = adam(n, *[[t[i] for i in groups[k]] for t in (w, m, v)], g, made[k], 5 if k < 4 else 9)

        sums, late = {}, []

        def due(keys, *inputs):
            got = order(*(sums[k] for k in keys), *inputs)
            sums.update(zip(keys, got))
            return got[len(keys) :]

        for n in reversed(range(layers)):
            wqkv, wo, wg, wu, wd = full[n]
            h, a, sa, qkv, o, lse, h1, b, sb, gate, up, act = kept[n]
            gwd, d, act = order(_dot(act, d, 0, 0).astype(BF), d, act)
            sums[n, 4] = summed(gwd)
            dact = _dot(d, wd, 1, 1).astype(BF).astype(F32)
            sig = jax.nn.sigmoid(gate)
            dup = (dact * (gate * sig)).astype(BF)
            dgate = (dact * up * (sig * (1 + gate * (1 - sig)))).astype(BF)
            dgate, dup = order(dgate, dup)
            dgate, dup = due(late, dgate, dup)
            gwg, dgate, dup = order(_dot(b, dgate, 0, 0).astype(BF), dgate, dup)
            sums[n, 2] = summed(gwg)
            gwu, dgate, dup = order(_dot(b, dup, 0, 0).astype(BF), dgate, dup)
            sums[n, 3] = summed(gwu)
            dgate, dup = due([(n, 4)], dgate, dup)
            db = _dot(dgate, wg, 1, 1) + _dot(dup, wu, 1, 1)
            d1 = d + by_norm(h1, sb, db)
            gwo, d1 = order(_dot(o, d1, 0, 0).astype(BF), d1)
            sums[n, 1] = summed(gwo)
            do = _dot(d1, wo, 1, 1).astype(BF)
            (do,) = due([(n, 2)], do)
            dqkv = attend_bwd(qkv, o, do, lse, cos, sin)
            (dqkv,) = due([(n, 3)], dqkv)
            gq, dqkv = order(_dot(a, dqkv, 0, 0).astype(BF), dqkv)
            sums[n, 0] = summed(gq)
            late = [(n, 1), (n, 0)]
            if n > 0:
                da = _dot(dqkv, wqkv, 1, 1)
                d = d1 + by_norm(h, sa, da)
        for n in reversed(range(layers)):
            for k in (4, 2, 3, 1, 0):
                take(n, k, sums[n, k])
        flat = {i: [made[k][t * len(groups[k]) + j] for t in range(3)] for k in range(5) for j, i in enumerate(groups[k])}
        return tuple(flat[i][t] for t in range(3) for i in range(7))

    states, cut = P(("rep", "dp"), None, None), P(None, "dp", None)
    return jax.shard_map(
        step,
        mesh=mesh,
        in_specs=(states, states) + (cut,) * 21,
        out_specs=(P("rep", "dp", None),) * 21,
        check_vma=False,
    )
```

```python
import functools

import jax
import jax.numpy as jnp
from jax import lax
from jax.experimental import pallas as pl
from jax.experimental.pallas import tpu as pltpu
from jax.sharding import PartitionSpec as P

HEAD = 128
THETA = 10000
HEADS, KV = 10, 2
GROUP = HEADS // KV
LOG2E = 1.4426950408889634
NEG = -1e30
HIDDEN = 2 * NEG
VMEM = 60 * 2**20
BF, F32 = jnp.bfloat16, jnp.float32
QW, KW = HEADS * HEAD, KV * HEAD


def _dot(a, b, ca, cb):
    return lax.dot_general(a, b, (((ca,), (cb,)), ((), ())), preferred_element_type=F32)


def _turn(x, cos, sin):
    x = x.astype(F32)
    return x * cos + pltpu.roll(x, HEAD // 2, 1) * sin


def _turn_back(x, cos, sin):
    x = x.astype(F32)
    return x * cos - pltpu.roll(x, HEAD // 2, 1) * sin


def _head(ref, n):
    return ref[:, n * HEAD : (n + 1) * HEAD]


def _gap(bk, cols, bq):
    return lax.rem(lax.broadcasted_iota(jnp.int32, (bk, cols), 1), bq) - lax.broadcasted_iota(jnp.int32, (bk, cols), 0)


def _load_keys(k_ref, ck_ref, sk_ref, k_s):
    for i in range(KV):
        k_s[i] = _turn(_head(k_ref, i), ck_ref[...], sk_ref[...]).astype(BF)


def _load_queries(q_ref, cq_ref, sq_ref, q_s, bq):
    for i in range(KV):
        for n in range(GROUP):
            q_s[i, n * bq : (n + 1) * bq, :] = _turn(_head(q_ref, i * GROUP + n), cq_ref[...], sq_ref[...]).astype(BF)


def _attn_fwd(q_ref, k_ref, v_ref, cq_ref, sq_ref, ck_ref, sk_ref, o_ref, lse_ref, q_s, k_s, v_s, top_s, mix_s, gap_s, *, bq, bk, wide):
    cols, s = GROUP * bq, k_ref.shape[0]
    iq = pl.program_id(0)
    scale = HEAD**-0.5
    e = scale * LOG2E
    pieces = [(i, at) for i in range(KV) for at in range(0, cols, wide)]

    @pl.when(iq == 0)
    def _():
        gap_s[...] = _gap(bk, cols, bq)
        _load_keys(k_ref, ck_ref, sk_ref, k_s)
        for i in range(KV):
            v_s[i, :HEAD, :] = _head(v_ref, i).T
            v_s[i, HEAD:, :] = jnp.ones((8, s), BF)

    _load_queries(q_ref, cq_ref, sq_ref, q_s, bq)
    top_s[...] = jnp.full(top_s.shape, NEG, F32)
    mix_s[...] = jnp.zeros(mix_s.shape, F32)

    def block(j, masked):
        here = pl.ds(pl.multiple_of(j * bk, bk), bk)
        scores = [_dot(k_s[i, here, :], q_s[i, at : at + wide, :], 1, 1) for i, at in pieces]
        if masked:
            ok = gap_s[...] >= j * bk - iq * bq
        weights, keeps = [], []
        for (i, at), x in zip(pieces, scores):
            if masked:
                x = jnp.where(ok[:, at : at + wide], x, HIDDEN)
            old = top_s[i : i + 1, at : at + wide]
            top = jnp.maximum(old, x.max(axis=0, keepdims=True))
            top_s[i : i + 1, at : at + wide] = top
            weights.append(jnp.exp2((x - top) * e).astype(BF))
            keeps.append(jnp.exp2((old - top) * e))
        for (i, at), p, keep in zip(pieces, weights, keeps):
            mix_s[i, :, at : at + wide] = mix_s[i, :, at : at + wide] * keep + _dot(v_s[i, :, here], p, 1, 0)

    whole, last = lax.div(iq * bq, bk), lax.div(iq * bq + bq + bk - 1, bk)
    lax.fori_loop(0, whole, lambda j, _: block(j, False), None)
    lax.fori_loop(whole, last, lambda j, _: block(j, True), None)

    for i in range(KV):
        top, total = top_s[i : i + 1, :], mix_s[i, HEAD : HEAD + 1, :]
        out = (mix_s[i, :HEAD, :] * (1 / total)).T.astype(BF)
        lse = top * scale + jnp.log(total)
        for n in range(GROUP):
            at = i * GROUP + n
            o_ref[:, at * HEAD : (at + 1) * HEAD] = out[n * bq : (n + 1) * bq, :]
            lse_ref[at : at + 1, :] = lse[:, n * bq : (n + 1) * bq]


def _attn_bwd(q_ref, k_ref, v_ref, o_ref, do_ref, lse_ref, cq_ref, sq_ref, ck_ref, sk_ref, d_ref, q_s, do_s, k_s, kt_s, dq_s, dk_s, dv_s, gap_s,
              *, bq, bk, wide):
    cols = GROUP * bq
    iq = pl.program_id(0)
    scale = HEAD**-0.5
    e = scale * LOG2E
    pieces = [(i, at) for i in range(KV) for at in range(0, cols, wide)]

    @pl.when(iq == 0)
    def _():
        gap_s[...] = _gap(bk, cols, bq)
        dk_s[...] = jnp.zeros_like(dk_s)
        dv_s[...] = jnp.zeros_like(dv_s)
        _load_keys(k_ref, ck_ref, sk_ref, k_s)
        for i in range(KV):
            kt_s[i] = k_s[i].T

    _load_queries(q_ref, cq_ref, sq_ref, q_s, bq)
    dq_s[...] = jnp.zeros_like(dq_s)
    lses, deltas = [], []
    for i in range(KV):
        row, delta = [], []
        for n in range(GROUP):
            at = i * GROUP + n
            do = _head(do_ref, at)
            do_s[i, n * bq : (n + 1) * bq, :] = do
            row.append(lse_ref[at : at + 1, :] * LOG2E)
            delta.append((do.astype(F32) * _head(o_ref, at).astype(F32)).T.sum(axis=0, keepdims=True))
        lses.append(jnp.concatenate(row, axis=1))
        deltas.append(jnp.concatenate(delta, axis=1))

    def block(j, masked):
        here = pl.ds(pl.multiple_of(j * bk, bk), bk)
        qs = [q_s[i, at : at + wide, :] for i, at in pieces]
        dos = [do_s[i, at : at + wide, :] for i, at in pieces]
        scores = [_dot(k_s[i, here, :], x, 1, 1) for (i, _), x in zip(pieces, qs)]
        dps = [_dot(v_ref[here, i * HEAD : (i + 1) * HEAD], x, 1, 1) for (i, _), x in zip(pieces, dos)]
        if masked:
            ok = gap_s[...] >= j * bk - iq * bq
        for n, (i, at) in enumerate(pieces):
            p = jnp.exp2(scores[n] * e - lses[i][:, at : at + wide])
            if masked:
                p = jnp.where(ok[:, at : at + wide], p, 0.0)
            ds = (p * (dps[n] - deltas[i][:, at : at + wide])).astype(BF)
            dv_s[i, here, :] += _dot(p.astype(BF), dos[n], 1, 0)
            dk_s[i, here, :] += _dot(ds, qs[n], 1, 0)
            dq_s[i, :, at : at + wide] += _dot(kt_s[i, :, here], ds, 1, 0)

    whole, last = lax.div(iq * bq, bk), lax.div(iq * bq + bq + bk - 1, bk)
    lax.fori_loop(0, whole, lambda j, _: block(j, False), None)
    lax.fori_loop(whole, last, lambda j, _: block(j, True), None)
    rows = pl.ds(pl.multiple_of(iq * bq, bq), bq)
    for i in range(KV):
        dq = (dq_s[i] * scale).T.astype(BF)
        for n in range(GROUP):
            at = i * GROUP + n
            d_ref[rows, at * HEAD : (at + 1) * HEAD] = _turn_back(dq[n * bq : (n + 1) * bq, :], cq_ref[...], sq_ref[...]).astype(BF)

    @pl.when(iq == pl.num_programs(0) - 1)
    def _():
        for i in range(KV):
            dk = (dk_s[i] * scale).astype(BF)
            d_ref[:, QW + i * HEAD : QW + (i + 1) * HEAD] = _turn_back(dk, ck_ref[...], sk_ref[...]).astype(BF)
            d_ref[:, QW + KW + i * HEAD : QW + KW + (i + 1) * HEAD] = dv_s[i].astype(BF)


def _attn_specs(s, bq):
    q = pl.BlockSpec((bq, QW), lambda i: (i, 0))
    k = pl.BlockSpec((s, KW), lambda i: (0, QW // KW))
    v = pl.BlockSpec((s, KW), lambda i: (0, QW // KW + 1))
    part = pl.BlockSpec((bq, HEAD), lambda i: (i, 0))
    whole = pl.BlockSpec((s, HEAD), lambda i: (0, 0))
    stat = pl.BlockSpec((HEADS, bq), lambda i: (0, i))
    return q, k, v, part, whole, stat


def attend(qkv, cos, sin, bq=512, bk=512, wide=512):
    s = qkv.shape[0]
    q, k, v, part, whole, stat = _attn_specs(s, bq)
    cols = GROUP * bq
    return pl.pallas_call(
        functools.partial(_attn_fwd, bq=bq, bk=bk, wide=wide),
        grid=(s // bq,),
        in_specs=[q, k, v, part, part, whole, whole],
        out_specs=[q, stat],
        out_shape=[jax.ShapeDtypeStruct((s, QW), BF), jax.ShapeDtypeStruct((HEADS, s), F32)],
        scratch_shapes=[pltpu.VMEM((KV, cols, HEAD), BF), pltpu.VMEM((KV, s, HEAD), BF), pltpu.VMEM((KV, HEAD + 8, s), BF),
                        pltpu.VMEM((KV, cols), F32), pltpu.VMEM((KV, HEAD + 8, cols), F32), pltpu.VMEM((bk, cols), jnp.int32)],
        compiler_params=pltpu.CompilerParams(dimension_semantics=("arbitrary",), vmem_limit_bytes=VMEM),
        cost_estimate=pl.CostEstimate(flops=40 * 10**9, transcendentals=HEADS * s * s, bytes_accessed=8 * s * QW),
        name="attend",
    )(qkv, qkv, qkv, cos, sin, cos, sin)


def attend_bwd(qkv, o, do, lse, cos, sin, bq=256, bk=256, wide=256):
    s = qkv.shape[0]
    q, k, v, part, whole, stat = _attn_specs(s, bq)
    cols = GROUP * bq
    return pl.pallas_call(
        functools.partial(_attn_bwd, bq=bq, bk=bk, wide=wide),
        grid=(s // bq,),
        in_specs=[q, k, v, q, q, stat, part, part, whole, whole],
        out_specs=pl.BlockSpec((s, QW + 2 * KW), lambda i: (0, 0)),
        out_shape=jax.ShapeDtypeStruct((s, QW + 2 * KW), BF),
        scratch_shapes=[pltpu.VMEM((KV, cols, HEAD), BF), pltpu.VMEM((KV, cols, HEAD), BF), pltpu.VMEM((KV, s, HEAD), BF),
                        pltpu.VMEM((KV, HEAD, s), BF), pltpu.VMEM((KV, HEAD, cols), F32), pltpu.VMEM((KV, s, HEAD), F32),
                        pltpu.VMEM((KV, s, HEAD), F32), pltpu.VMEM((bk, cols), jnp.int32)],
        compiler_params=pltpu.CompilerParams(dimension_semantics=("arbitrary",), vmem_limit_bytes=VMEM),
        cost_estimate=pl.CostEstimate(flops=80 * 10**9, transcendentals=HEADS * s * s, bytes_accessed=16 * s * QW),
        name="attend_bwd",
    )(qkv, qkv, qkv, o, do, lse, cos, sin, cos, sin)


def _adam(count, *refs):
    ws, ms, vs, gs = (refs[i * count : (i + 1) * count] for i in range(4))
    outs = refs[-3 * count :]
    for i in range(count):
        g = gs[i][...].astype(F32)
        w = ws[i][0].astype(F32)
        m = 0.9 * ms[i][0] + 0.1 * g
        v = 0.95 * vs[i][0] + 0.05 * g * g
        outs[i][0] = (w - 0.02 * (m * lax.rsqrt(v + 1e-8) + 0.1 * w)).astype(BF)
        outs[count + i][0] = m
        outs[2 * count + i][0] = v


def adam(number, ws, ms, vs, g, made, steps):
    count, rows = len(ws), g.shape[0]
    br = rows // steps
    layer = [pl.BlockSpec((1, br, w.shape[2]), lambda i: (number, i, 0)) for w in ws]
    at, gspecs = 0, []
    for w in ws:
        n = w.shape[2]
        gspecs.append(pl.BlockSpec((br, n), functools.partial(lambda i, c: (i, c), c=at // n)))
        at += n
    made = () if made is None else made
    elements = rows * at
    return pl.pallas_call(
        functools.partial(_adam, count),
        grid=(steps,),
        in_specs=layer * 3 + gspecs + [pl.BlockSpec(memory_space=pl.ANY)] * len(made),
        out_specs=layer * 3,
        out_shape=[jax.ShapeDtypeStruct(w.shape, t) for t in (BF, F32, F32) for w in ws],
        input_output_aliases={4 * count + i: i for i in range(len(made))},
        compiler_params=pltpu.CompilerParams(dimension_semantics=("arbitrary",), vmem_limit_bytes=40 * 2**20),
        cost_estimate=pl.CostEstimate(flops=2000 * elements, transcendentals=elements, bytes_accessed=22 * elements),
        name="adam",
    )(*ws, *ms, *vs, *([g] * count), *made)


def matmul(a, w):
    return jnp.dot(a, w, preferred_element_type=F32).astype(BF)


def normed(h):
    wide = h.astype(F32)
    scale = lax.rsqrt(jnp.mean(wide**2, -1, keepdims=True) + 1e-6)
    return (wide * scale).astype(BF), scale


def by_norm(h, scale, d):
    wide, d = h.astype(F32), d.astype(F32)
    return (scale * d - wide * (scale**3 * jnp.mean(wide * d, -1, keepdims=True))).astype(BF)


def order(*arrays):
    return lax.optimization_barrier(arrays)


def solution(mesh):
    def whole(shard):
        half = shard.shape[0] // 2
        mine = lax.dynamic_slice_in_dim(shard, lax.axis_index("rep") * half, half, 0)
        return lax.all_gather(mine, ("dp", "rep"), axis=0, tiled=True)

    ACROSS = [(0, 2), (2, 0), (1, 3), (3, 1)]
    BESIDE = [(0, 1), (1, 0), (2, 3), (3, 2)]

    def joined(shard, first, second, pieces):
        rows, half = shard.shape[0], shard.shape[0] // 2
        r, me = lax.axis_index("rep"), lax.axis_index("dp")
        across, other, far = (me + 2) % 4, me + 1 - 2 * (me % 2), (me + 3 - 2 * (me % 2)) % 4
        out = jnp.zeros((4 * rows, shard.shape[1]), BF)
        for piece, at in zip((shard, pieces[0], first, pieces[1], second, pieces[2]),
                             (me * rows, other * rows, across * rows + r * half, far * rows + r * half, across * rows + half - r * half,
                              far * rows + half - r * half)):
            out = lax.dynamic_update_slice_in_dim(out, piece, at, 0)
        return out

    def summed(g):
        return lax.psum_scatter(g, "dp", scatter_dimension=0, tiled=True)

    def step(x, dy, *arrays):
        w, m, v = (arrays[i : i + 7] for i in (0, 7, 14))
        layers = w[0].shape[0]
        tokens = x.shape[1]
        freq = THETA ** (-jnp.arange(HEAD // 2, dtype=F32) / (HEAD // 2))
        angle = jnp.arange(tokens, dtype=F32)[:, None] * freq
        cos, sin = jnp.cos(angle), jnp.sin(angle)
        cos, sin = jnp.concatenate([cos, cos], 1), jnp.concatenate([-sin, sin], 1)

        full = []
        for n in range(layers):
            qkv = jnp.concatenate([w[0][n], w[1][n], w[2][n]], axis=1)
            full.append([whole(qkv), whole(w[3][n]), whole(w[4][n]), w[5][n], whole(w[6][n])])

        h, kept = x[0], []
        for n in range(layers):
            wqkv, wo, wg, shard, wd = full[n]
            half = shard.shape[0] // 2
            wqkv, h, shard = order(wqkv, h, shard)
            mine = lax.dynamic_slice_in_dim(shard, lax.axis_index("rep") * half, half, 0)
            first, near = lax.ppermute(mine, "dp", ACROSS), lax.ppermute(shard, "dp", BESIDE)
            a, sa = normed(h)
            qkv = matmul(a, wqkv)
            o, lse = attend(qkv, cos, sin)
            o, first, near = order(o, first, near)
            second, near_first = lax.ppermute(first, "rep", [(0, 1), (1, 0)]), lax.ppermute(first, "dp", BESIDE)
            h1 = h + matmul(o, wo)
            b, sb = normed(h1)
            gate = jnp.dot(b, wg, preferred_element_type=F32)
            gate, second, near_first = order(gate, second, near_first)
            wu = joined(shard, first, second, (near, near_first, lax.ppermute(second, "dp", BESIDE)))
            full[n][3] = wu
            up = jnp.dot(b, wu, preferred_element_type=F32)
            act = (jax.nn.silu(gate) * up).astype(BF)
            kept.append((h, a, sa, qkv, o, lse, h1, b, sb, gate, up, act))
            if n < layers - 1:
                h = h1 + matmul(act, wd)

        d = dy[0]
        made = [None] * 5
        groups = [(0, 1, 2), (3,), (4,), (5,), (6,)]

        def take(n, k, g):
            made[k] = adam(n, *[[t[i] for i in groups[k]] for t in (w, m, v)], g, made[k], 5 if k < 4 else 9)

        sums, late = {}, []

        def due(keys, *inputs):
            got = order(*(sums[k] for k in keys), *inputs)
            sums.update(zip(keys, got))
            return got[len(keys) :]

        for n in reversed(range(layers)):
            wqkv, wo, wg, wu, wd = full[n]
            h, a, sa, qkv, o, lse, h1, b, sb, gate, up, act = kept[n]
            gwd, d, act = order(_dot(act, d, 0, 0).astype(BF), d, act)
            sums[n, 4] = summed(gwd)
            dact = _dot(d, wd, 1, 1).astype(BF).astype(F32)
            sig = jax.nn.sigmoid(gate)
            dup = (dact * (gate * sig)).astype(BF)
            dgate = (dact * up * (sig * (1 + gate * (1 - sig)))).astype(BF)
            dgate, dup = order(dgate, dup)
            dgate, dup = due(late, dgate, dup)
            gwg, dgate, dup = order(_dot(b, dgate, 0, 0).astype(BF), dgate, dup)
            sums[n, 2] = summed(gwg)
            gwu, dgate, dup = order(_dot(b, dup, 0, 0).astype(BF), dgate, dup)
            sums[n, 3] = summed(gwu)
            dgate, dup = due([(n, 4)], dgate, dup)
            db = _dot(dgate, wg, 1, 1) + _dot(dup, wu, 1, 1)
            d1 = d + by_norm(h1, sb, db)
            gwo, d1 = order(_dot(o, d1, 0, 0).astype(BF), d1)
            sums[n, 1] = summed(gwo)
            do = _dot(d1, wo, 1, 1).astype(BF)
            (do,) = due([(n, 2)], do)
            dqkv = attend_bwd(qkv, o, do, lse, cos, sin)
            (dqkv,) = due([(n, 3)], dqkv)
            gq, dqkv = order(_dot(a, dqkv, 0, 0).astype(BF), dqkv)
            sums[n, 0] = summed(gq)
            late = [(n, 1), (n, 0)]
            if n > 0:
                da = _dot(dqkv, wqkv, 1, 1)
                d = d1 + by_norm(h, sa, da)
        for n in reversed(range(layers)):
            for k in (4, 2, 3, 1, 0):
                take(n, k, sums[n, k])
        flat = {i: [made[k][t * len(groups[k]) + j] for t in range(3)] for k in range(5) for j, i in enumerate(groups[k])}
        return tuple(flat[i][t] for t in range(3) for i in range(7))

    states, cut = P(("rep", "dp"), None, None), P(None, "dp", None)
    return jax.shard_map(
        step,
        mesh=mesh,
        in_specs=(states, states) + (cut,) * 21,
        out_specs=(P("rep", "dp", None),) * 21,
        check_vma=False,
    )
```
